512 devices in a mesh: tok: 8 (over x, core), vocab: 64 (over z, y).
Axes of the slice: x: 4, y: 4, z: 16, core: 2. Of those that a mesh axis runs over, the one named last changes fastest.
Arguments:
- hidden: bfloat16 [6144, 4096], P('tok', 'vocab'), as said below
- weight: bfloat16 [4096, 65536], P('tok', 'vocab'), may hold values from -0.09375 to 0.09375
- targets: int32 [6144], P('tok'), may hold values from 0 to 65535
- domains: int32 [6144], P('tok'), may hold values from 0 to 63
- seq_len: int32 [48], P('tok'), may hold values from 1 to 128
Outputs:
- token_loss: float32 [6144], P(('tok', 'vocab'))
- domain_mean: float32 [64], replicated
The draws below stay inside these ranges and needn't reach their ends.
Inputs may be any that keep to these rules, and one draw needn't show every extreme that they name: hidden states of the eval window.
All inputs are finite; a program needn't handle non-finite values.
Results may differ from the reference program's by a relative error of at most 0.0003.
Values may be sent and summed in bfloat16 or wider, within the bound.
No kernel may reach another device: no remote copies, remote signals or barrier semaphores. Data moves between devices by JAX's collectives and lax.ppermute only.
A program may use at most 64 MiB of HBM per device.

```python
import math
import jax
import jax.numpy as jnp
import numpy as np
from jax import lax

D = 4096
VOCAB = 65536
TOK_DEV = 768
SEQ_LEN = 128
DOMAINS = 64
TOKENS = 6144
SEQS = 48


def draw_hidden(key, part):
    values = jax.random.normal(key, (TOKENS, D), jnp.float32) * 3.0
    return values.astype(jnp.bfloat16)


def set_ends(values, rng, low, top_value):
    index_at = [jax.random.randint(jax.random.fold_in(rng, axis), (), 0, length) for axis, length in enumerate(values.shape)]
    longest = values.shape.index(max(values.shape))
    next_to = index_at[:longest] + [(index_at[longest] + 1) % values.shape[longest]] + index_at[longest + 1:]
    return values.at[tuple(index_at)].set(low).at[tuple(next_to)].set(top_value)


def levels(own_key, extent, cuts, least, high):
    def one(position, shards_of):
        steps = jax.random.uniform(jax.random.fold_in(jax.random.fold_in(own_key, 6), position), (shards_of,), jnp.float32, least / len(cuts), high / len(cuts))
        return jnp.repeat(jnp.exp(steps), extent[position] // shards_of).reshape((-1,) + (1,) * (len(extent) - position - 1))

    loudness = one(*cuts[0])
    for cut in cuts[1:]:
        loudness = loudness * one(*cut)
    return loudness


def cumulative_ranks(number_of, lean):
    portions = [(1 << 20) // math.isqrt(rank ** lean) + 1 for rank in range(1, number_of + 1)]
    deviation = 1 + sum(portions) // (1 << 30)
    return np.cumsum(np.array([max(1, weight // deviation) for weight in portions]))


def ranked_ids(stream_key, shape, count, skew):
    table = cumulative_ranks(count, skew)
    ticket = jax.random.randint(jax.random.fold_in(stream_key, 1), shape, 0, int(table[count - 1]))
    standing = jnp.searchsorted(jnp.asarray(table, jnp.int32), ticket, side="right")
    return jax.random.permutation(jax.random.fold_in(stream_key, 2), count)[standing].astype(jnp.int32)


def noise(key, dims, spread, limit, shards=(), kind=jnp.bfloat16):
    result = spread * jax.random.normal(key, dims, jnp.float32)
    if shards:
        result = result * levels(key, dims, shards, -0.22, 0.18)
    return jnp.clip(result, -limit, limit).astype(kind)


def setup_inputs(seed: int = 0) -> dict:
    seeds = jax.random.split(jax.random.key(seed), 6)
    return {
        "hidden": draw_hidden(jax.random.fold_in(seeds[5], 71), 0),
        "weight": noise(seeds[1], (D, VOCAB), D ** -0.5, 0.09375, ((0, 8), (1, 64))),
        "targets": set_ends(ranked_ids(seeds[2], (TOKENS,), VOCAB, 2), jax.random.fold_in(seeds[2], 3), 0, VOCAB - 1).astype(jnp.int32),
        "domains": set_ends(jax.random.randint(seeds[3], (TOKENS,), 0, DOMAINS), jax.random.fold_in(seeds[3], 1), 0, DOMAINS - 1).astype(jnp.int32),
        "seq_len": set_ends(jax.random.randint(seeds[4], (SEQS,), 1, SEQ_LEN + 1), jax.random.fold_in(seeds[4], 1), 1, SEQ_LEN).astype(jnp.int32),
    }


def block_stats(pair):
    rows, wanted = pair
    logits = jnp.dot(rows, WEIGHT_HOLDER[0], preferred_element_type=jnp.float32)
    row_top = jnp.max(logits, axis=1)
    row_total = jnp.sum(jnp.exp(logits - row_top[:, None]), axis=1)
    picked = jnp.take_along_axis(logits, wanted[:, None].astype(jnp.int32), axis=1)[:, 0]
    return row_top, row_total, picked


WEIGHT_HOLDER = []


def reference(hidden, weight, targets, domains, seq_len):
    blocks = TOKENS // TOK_DEV

    def block_fn(pair):
        rows, wanted = pair
        logits = jnp.dot(rows, weight, preferred_element_type=jnp.float32)
        row_top = jnp.max(logits, axis=1)
        row_total = jnp.sum(jnp.exp(logits - row_top[:, None]), axis=1)
        picked = jnp.take_along_axis(logits, wanted[:, None].astype(jnp.int32), axis=1)[:, 0]
        return row_top, row_total, picked

    row_top, row_total, picked = lax.map(block_fn, (hidden.reshape(blocks, TOK_DEV, D), targets.reshape(blocks, TOK_DEV)))
    row_top = row_top.reshape(TOKENS)
    row_total = row_total.reshape(TOKENS)
    picked = picked.reshape(TOKENS)
    positions = jnp.arange(TOKENS, dtype=jnp.int32)
    lengths = seq_len[positions // SEQ_LEN]
    valid_mask = ((positions % SEQ_LEN) < lengths).astype(jnp.float32)
    token_loss = (jnp.log(row_total) + row_top - picked) * valid_mask
    onehot = (domains[:, None] == jnp.arange(DOMAINS, dtype=jnp.int32)[None, :]).astype(jnp.float32)
    domain_sum = jnp.dot(token_loss, onehot, precision=lax.Precision.HIGHEST)
    domain_count = jnp.dot(valid_mask, onehot, precision=lax.Precision.HIGHEST)
    domain_mean = domain_sum / jnp.maximum(domain_count, 1.0)
    return token_loss, domain_mean
```

```python
import jax
import jax.numpy as jnp
from jax import lax
from jax.sharding import Mesh
from jax.sharding import PartitionSpec as P

SEQ_LEN = 128
DOMAINS = 64
TOK = ("x", "c")
VOCAB = ("z", "y")
SWAP = [(0, 1), (1, 0)]


def to_all(array, axis, copies):
    return lax.all_to_all(
        jnp.broadcast_to(array[None], (copies, *array.shape)), axis, 0, 0, tiled=True
    )


def gathered_weight(weight):
    core = lax.axis_index("c")
    half = weight.shape[1] // 2
    keep = lax.dynamic_slice_in_dim(weight, core * half, half, 1)
    give = lax.dynamic_slice_in_dim(weight, (1 - core) * half, half, 1)
    other = lax.ppermute(give, "c", SWAP)
    rows = jnp.where(
        core == 0, jnp.concatenate([keep, other], 0), jnp.concatenate([other, keep], 0)
    )
    chips = lax.axis_size("x")
    own = to_all(rows, "x", chips).reshape(chips * rows.shape[0], half)
    return own, lax.ppermute(own, "c", SWAP)


def tail(lse, picked, domains, seq_len):
    tokens = lse.shape[0]
    zs, ys = lax.axis_size("z"), lax.axis_size("y")
    own = tokens // (zs * ys)
    y = lax.axis_index("y")
    slices = jnp.stack([lse, picked]).reshape(2, zs, ys, own).transpose(2, 0, 1, 3)
    send = jnp.broadcast_to(slices.reshape(1, ys, -1), (zs, ys, 2 * zs * own))
    got = lax.all_to_all(send.reshape(zs * ys, -1), VOCAB, 0, 0, tiled=True)
    got = got.reshape(zs * ys, 2, zs * own)
    top = jnp.max(got[:, 0], axis=0)
    total = jnp.sum(jnp.exp(got[:, 0] - top[None]), axis=0)
    raw = jnp.log(total) + top - jnp.sum(got[:, 1], axis=0)
    index = lax.iota(jnp.int32, zs * own)
    local = (index // own) * (ys * own) + y * own + index % own
    seqs = seq_len.shape[0]
    lengths = jnp.sum(
        jnp.where((local // SEQ_LEN)[:, None] == lax.broadcasted_iota(jnp.int32, (zs * own, seqs), 1), seq_len[None], 0),
        axis=1,
    )
    mask = (local % SEQ_LEN < lengths).astype(jnp.float32)
    loss = raw * mask
    domain = lax.dynamic_index_in_dim(domains.reshape(zs, ys, own), y, 1, False).reshape(-1)
    here = domain[None, :] == lax.broadcasted_iota(jnp.int32, (DOMAINS, zs * own), 0)
    sums = jnp.sum(jnp.where(here, loss[None], 0.0), axis=1)
    counts = jnp.sum(jnp.where(here, mask[None], 0.0), axis=1)
    part = jnp.concatenate([sums, counts])
    axes = ("x", "c", "y")
    whole = jnp.sum(to_all(part, axes, lax.axis_size(axes)), axis=0)
    mean = whole[:DOMAINS] / jnp.maximum(whole[DOMAINS:], 1.0)
    token_loss = lax.dynamic_index_in_dim(loss.reshape(zs, own), lax.axis_index("z"), 0, False)
    return token_loss, mean


def body(hidden, weight, targets, domains, seq_len):
    features = lax.all_gather(hidden, "y", axis=1, tiled=True)
    features = lax.all_gather(features, "z", axis=1, tiled=True)
    core = lax.axis_index("c")
    halves = gathered_weight(weight)
    columns = weight.shape[1]
    half = columns // 2
    first = lax.axis_index(VOCAB) * columns
    logits = [jnp.dot(features, w, preferred_element_type=jnp.float32) for w in halves]
    tops = jnp.maximum(jnp.max(logits[0], axis=1), jnp.max(logits[1], axis=1))
    total, picked = 0.0, 0.0
    for values, start in zip(logits, (core * half, (1 - core) * half)):
        ids = first + start + lax.broadcasted_iota(jnp.int32, values.shape, 1)
        total += jnp.sum(jnp.exp(values - tops[:, None]), axis=1)
        picked += jnp.sum(jnp.where(ids == targets[:, None], values, 0.0), axis=1)
    return tail(jnp.log(total) + tops, picked, domains, seq_len)


def solution(mesh):
    split = Mesh(mesh.devices.reshape(4, 2, 16, 4), ("x", "c", "z", "y"))
    placed = (P(TOK, VOCAB), P(TOK, VOCAB), P(TOK), P(TOK), P(TOK))
    return jax.shard_map(
        body, mesh=split, in_specs=placed, out_specs=(P((*TOK, *VOCAB)), P()), check_vma=False
    )
```

```python
import jax
import jax.numpy as jnp
from jax import lax
from jax.experimental import pallas as pl
from jax.experimental.pallas import tpu as pltpu
from jax.sharding import Mesh
from jax.sharding import PartitionSpec as P


SEQ_LEN = 128
DOMAINS = 64
TOK = ("x", "c")
VOCAB = ("z", "y")
SWAP = [(0, 1), (1, 0)]
BLOCK = 256
TILE = 256
BATCHES = ((1, 2, 3), (4, 5, 6), (7,))
GROUPS = ((range(0, 7), (0,)), ((7, 8), (1, 2)))


def to_all(array, axis, copies):
    return lax.all_to_all(
        jnp.broadcast_to(array[None], (copies, *array.shape)), axis, 0, 0, tiled=True
    )


def gathered_weight(weight):
    core = lax.axis_index("c")
    half = weight.shape[1] // 2
    keep = lax.dynamic_slice_in_dim(weight, core * half, half, 1)
    give = lax.dynamic_slice_in_dim(weight, (1 - core) * half, half, 1)
    other = lax.ppermute(give, "c", SWAP)
    rows = jnp.where(
        core == 0, jnp.concatenate([keep, other], 0), jnp.concatenate([other, keep], 0)
    )
    chips = lax.axis_size("x")
    own = to_all(rows, "x", chips)
    own = own.reshape(chips * rows.shape[0], half)
    swapped = lax.ppermute(own, "c", SWAP)
    return own, swapped


def tail(lse, picked, domains, seq_len):
    tokens = lse.shape[0]
    zs, ys = lax.axis_size("z"), lax.axis_size("y")
    own = tokens // (zs * ys)
    y = lax.axis_index("y")
    slices = jnp.stack([lse, picked]).reshape(2, zs, ys, own).transpose(2, 0, 1, 3)
    send = jnp.broadcast_to(slices.reshape(1, ys, -1), (zs, ys, 2 * zs * own))
    got = lax.all_to_all(send.reshape(zs * ys, -1), VOCAB, 0, 0, tiled=True)
    got = got.reshape(zs * ys, 2, zs * own)
    top = jnp.max(got[:, 0], axis=0)
    total = jnp.sum(jnp.exp(got[:, 0] - top[None]), axis=0)
    raw = jnp.log(total) + top - jnp.sum(got[:, 1], axis=0)
    index = lax.iota(jnp.int32, zs * own)
    local = (index // own) * (ys * own) + y * own + index % own
    seqs = seq_len.shape[0]
    lengths = jnp.sum(
        jnp.where((local // SEQ_LEN)[:, None] == lax.broadcasted_iota(jnp.int32, (zs * own, seqs), 1), seq_len[None], 0),
        axis=1,
    )
    mask = (local % SEQ_LEN < lengths).astype(jnp.float32)
    loss = raw * mask
    domain = lax.dynamic_index_in_dim(domains.reshape(zs, ys, own), y, 1, False).reshape(-1)
    here = domain[None, :] == lax.broadcasted_iota(jnp.int32, (DOMAINS, zs * own), 0)
    sums = jnp.sum(jnp.where(here, loss[None], 0.0), axis=1)
    counts = jnp.sum(jnp.where(here, mask[None], 0.0), axis=1)
    part = jnp.concatenate([sums, counts])
    axes = ("x", "c", "y")
    whole = jnp.sum(to_all(part, axes, lax.axis_size(axes)), axis=0)
    mean = whole[:DOMAINS] / jnp.maximum(whole[DOMAINS:], 1.0)
    token_loss = lax.dynamic_index_in_dim(loss.reshape(zs, own), lax.axis_index("z"), 0, False)
    return token_loss, mean


def product_kernel(stacks, first):
    def kernel(*refs):
        which, given, rest = refs[0], refs[1 : 1 + len(stacks)], refs[1 + len(stacks) :]
        blocks = [
            (ref,) if n is None else (ref, k)
            for ref, n in zip(given, stacks)
            for k in range(n or 1)
        ]
        count, tokens = len(blocks), given[0].shape[-2]
        halves, rest = rest[:2], rest[2:]
        if not first:
            before, rest = rest[:2], rest[2:]
        outs, (rows, sems) = rest[:2], rest[2:]
        copies = []
        for k in range(count):
            for h in range(2):
                copy = pltpu.make_async_copy(
                    halves[h].at[pl.ds(which[k] * BLOCK, BLOCK)], rows.at[k, h], sems.at[k, h]
                )
                copy.start()
                copies.append(copy)
        for copy in copies:
            copy.wait()
        for at in range(0, tokens, TILE):
            for h in range(2):
                total = None if first else before[h][at : at + TILE]
                for k in range(count):
                    ref, *at_k = blocks[k]
                    block = ref[(*at_k, slice(at, at + TILE))]
                    part = jnp.dot(block, rows[k, h], preferred_element_type=jnp.float32)
                    total = part if total is None else total + part
                outs[h][at : at + TILE] = total

    return kernel


def product(which, blocks, halves, before=None):
    tokens, depth = blocks[0].shape[-2:]
    half, arrays = halves[0].shape[1], len(blocks)
    stacks = [b.shape[0] if b.ndim == 3 else None for b in blocks]
    count = sum(n or 1 for n in stacks)
    vmem = pl.BlockSpec(memory_space=pltpu.VMEM)
    anywhere = pl.BlockSpec(memory_space=pl.ANY)
    shape = jax.ShapeDtypeStruct((tokens, half), jnp.float32)
    return pl.pallas_call(
        product_kernel(stacks, before is None),
        in_specs=[pl.BlockSpec(memory_space=pltpu.SMEM)]
        + [vmem] * arrays
        + [anywhere] * 2
        + ([] if before is None else [vmem] * 2),
        out_specs=[vmem, vmem],
        out_shape=[shape, shape],
        scratch_shapes=[
            pltpu.VMEM((count, 2, depth, half), jnp.bfloat16),
            pltpu.SemaphoreType.DMA((count, 2)),
        ],
        input_output_aliases={} if before is None else {3 + arrays: 0, 4 + arrays: 1},
        cost_estimate=pl.CostEstimate(
            flops=2 * count * tokens * depth * half * 2,
            bytes_accessed=count * depth * (tokens + 2 * half) * 2,
            transcendentals=0,
        ),
    )(which, *blocks, *halves, *(before or ()))


def along_z(array):
    zs = lax.axis_size("z")
    pairs = [(c * zs + z, c * zs + (z + (1 - 2 * c)) % zs) for c in range(2) for z in range(zs)]
    return lax.ppermute(array, ("c", "z"), pairs)


def loss(hidden, weight, targets, domains, seq_len):
    core, z = lax.axis_index("c"), lax.axis_index("z")
    zs, ys = lax.axis_size("z"), lax.axis_size("y")
    halves = gathered_weight(weight)
    mine = to_all(hidden.T, "y", ys).reshape(BLOCK, -1).T
    rings = zs // 2
    own, other = [mine], [lax.ppermute(mine, "c", SWAP)]
    for r in range(1, rings + 1):
        own.append(along_z(own[-1]))
        if r < rings:
            other.append(along_z(other[-1]))
    swapped = []
    for some in BATCHES:
        swapped.append(lax.ppermute(jnp.stack([other[r] for r in some]), "c", SWAP))
    step = 2 * core - 1
    logits = None
    for rounds, batches in GROUPS:
        away = [r for r in rounds] + [-r for k in batches for r in BATCHES[k]]
        which = lax.rem(z + step * jnp.array(away, jnp.int32) + zs, zs)
        blocks = [own[r] for r in rounds] + [swapped[k] for k in batches]
        logits = product(which, blocks, halves, logits)
    columns = weight.shape[1]
    half = columns // 2
    first = lax.axis_index(VOCAB) * columns
    tops = jnp.maximum(jnp.max(logits[0], axis=1), jnp.max(logits[1], axis=1))
    total, picked = 0.0, 0.0
    for values, start in zip(logits, (core * half, (1 - core) * half)):
        ids = first + start + lax.broadcasted_iota(jnp.int32, values.shape, 1)
        total += jnp.sum(jnp.exp(values - tops[:, None]), axis=1)
        picked += jnp.sum(jnp.where(ids == targets[:, None], values, 0.0), axis=1)
    return tail(jnp.log(total) + tops, picked, domains, seq_len)


def solution(mesh):
    split = Mesh(mesh.devices.reshape(4, 2, 16, 4), ("x", "c", "z", "y"))
    placed = (P(TOK, VOCAB), P(TOK, VOCAB), P(TOK), P(TOK), P(TOK))
    return jax.shard_map(
        loss, mesh=split, in_specs=placed, out_specs=(P((*TOK, *VOCAB)), P()), check_vma=False
    )
```

```python
import jax
import jax.numpy as jnp
from jax import lax
from jax.experimental import pallas as pl
from jax.experimental.pallas import tpu as pltpu
from jax.sharding import Mesh
from jax.sharding import PartitionSpec as P


SEQ_LEN = 128
DOMAINS = 64
TOK = ("x", "c")
VOCAB = ("z", "y")
SWAP = [(0, 1), (1, 0)]
BLOCK = 256
TILE = 256
LIMIT = 24 << 20
BATCHES = ((1, 2, 3), (4, 5, 6), (7,))
GROUPS = (
    ("early", range(0, 5), ()),
    ("middle", (5, 6, 7), (0,)),
    ("late", (8,), (1, 2)),
)


def to_all(array, axis, copies):
    return lax.all_to_all(
        jnp.broadcast_to(array[None], (copies, *array.shape)), axis, 0, 0, tiled=True
    )


def gathered_weight(weight):
    core = lax.axis_index("c")
    half = weight.shape[1] // 2
    keep = lax.dynamic_slice_in_dim(weight, core * half, half, 1)
    give = lax.dynamic_slice_in_dim(weight, (1 - core) * half, half, 1)
    other = lax.ppermute(give, "c", SWAP)
    rows = jnp.where(
        core == 0, jnp.concatenate([keep, other], 0), jnp.concatenate([other, keep], 0)
    )
    chips = lax.axis_size("x")
    own = to_all(rows, "x", chips)
    own = own.reshape(chips * rows.shape[0], half)
    swapped = lax.ppermute(own, "c", SWAP)
    return own, swapped


def tail(stats, domains, seq_len):
    tokens = stats.shape[1]
    zs, ys = lax.axis_size("z"), lax.axis_size("y")
    own = tokens // (zs * ys)
    y = lax.axis_index("y")
    slices = stats.reshape(2, zs, ys, own).transpose(2, 0, 1, 3)
    send = jnp.broadcast_to(slices.reshape(1, ys, -1), (zs, ys, 2 * zs * own))
    got = lax.all_to_all(send.reshape(zs * ys, -1), VOCAB, 0, 0, tiled=True)
    got = got.reshape(zs * ys, 2, zs * own)
    top = jnp.max(got[:, 0], axis=0)
    total = jnp.sum(jnp.exp(got[:, 0] - top[None]), axis=0)
    raw = jnp.log(total) + top - jnp.sum(got[:, 1], axis=0)
    index = lax.iota(jnp.int32, zs * own)
    local = (index // own) * (ys * own) + y * own + index % own
    seqs = seq_len.shape[0]
    lengths = jnp.sum(
        jnp.where((local // SEQ_LEN)[:, None] == lax.broadcasted_iota(jnp.int32, (zs * own, seqs), 1), seq_len[None], 0),
        axis=1,
    )
    mask = (local % SEQ_LEN < lengths).astype(jnp.float32)
    loss = raw * mask
    domain = lax.dynamic_index_in_dim(domains.reshape(zs, ys, own), y, 1, False).reshape(-1)
    here = domain[None, :] == lax.broadcasted_iota(jnp.int32, (DOMAINS, zs * own), 0)
    sums = jnp.sum(jnp.where(here, loss[None], 0.0), axis=1)
    counts = jnp.sum(jnp.where(here, mask[None], 0.0), axis=1)
    part = jnp.concatenate([sums, counts])
    axes = ("x", "c", "y")
    whole = jnp.sum(to_all(part, axes, lax.axis_size(axes)), axis=0)
    mean = whole[:DOMAINS] / jnp.maximum(whole[DOMAINS:], 1.0)
    token_loss = lax.dynamic_index_in_dim(loss.reshape(zs, own), lax.axis_index("z"), 0, False)
    return token_loss, mean


def product_kernel(stacks, first, last):
    def kernel(*refs):
        which, given, rest = refs[0], refs[1 : 1 + len(stacks)], refs[1 + len(stacks) :]
        blocks = [
            (ref,) if n is None else (ref, k)
            for ref, n in zip(given, stacks)
            for k in range(n or 1)
        ]
        count, tokens = len(blocks), given[0].shape[-2]
        halves, rest = rest[:2], rest[2:]
        if not first:
            before, rest = rest[:2], rest[2:]
        if last:
            wanted, rest = rest[0], rest[1:]
        *outs, rows, sems = rest
        copies = []
        for k in range(count):
            for h in range(2):
                copy = pltpu.make_async_copy(
                    halves[h].at[pl.ds(which[k] * BLOCK, BLOCK)], rows.at[k, h], sems.at[k, h]
                )
                copy.start()
                copies.append(copy)
        for copy in copies:
            copy.wait()
        for at in range(0, tokens, TILE):
            part = slice(at, at + TILE)
            totals = []
            for h in range(2):
                total = None if first else before[h][part]
                for k in range(count):
                    ref, *at_k = blocks[k]
                    more = jnp.dot(
                        ref[(*at_k, part)], rows[k, h], preferred_element_type=jnp.float32
                    )
                    total = more if total is None else total + more
                totals.append(total)
            if not last:
                outs[0][part], outs[1][part] = totals
                continue
            tops = [jnp.max(values, axis=1, keepdims=True) for values in totals]
            top = jnp.maximum(*tops)
            lane = lax.broadcasted_iota(jnp.int32, totals[0].shape, 1)
            total, picked = 0.0, 0.0
            for h, values in enumerate(totals):
                total += jnp.sum(jnp.exp(values - top), axis=1, keepdims=True)
                here = lane == wanted[part] - which[count + h]
                picked += jnp.sum(jnp.where(here, values, 0.0), axis=1, keepdims=True)
            lse = jnp.log(total) + top
            side = lax.broadcasted_iota(jnp.int32, (TILE, 128), 1)
            both = jnp.where(side == 0, lse, picked)
            outs[0][:, part] = both.T[:8]

    return kernel


def product(which, blocks, halves, before=None, wanted=None):
    tokens, depth = blocks[0].shape[-2:]
    half, arrays = halves[0].shape[1], len(blocks)
    stacks = [b.shape[0] if b.ndim == 3 else None for b in blocks]
    count = sum(n or 1 for n in stacks)
    last = wanted is not None
    vmem = pl.BlockSpec(memory_space=pltpu.VMEM)
    shape = jax.ShapeDtypeStruct((tokens, half), jnp.float32)
    extra = (before or ()) + ((wanted,) if last else ())
    aliases = {} if before is None or last else {3 + arrays: 0, 4 + arrays: 1}
    return pl.pallas_call(
        product_kernel(stacks, before is None, last),
        in_specs=[pl.BlockSpec(memory_space=pltpu.SMEM)]
        + [vmem] * arrays
        + [pl.BlockSpec(memory_space=pltpu.HBM)] * 2
        + [vmem] * len(extra),
        out_specs=vmem if last else [vmem, vmem],
        out_shape=jax.ShapeDtypeStruct((8, tokens), jnp.float32) if last else [shape, shape],
        scratch_shapes=[
            pltpu.VMEM((count, 2, depth, half), jnp.bfloat16),
            pltpu.SemaphoreType.DMA((count, 2)),
        ],
        input_output_aliases=aliases,
        compiler_params=pltpu.CompilerParams(vmem_limit_bytes=LIMIT),
        cost_estimate=pl.CostEstimate(
            flops=2 * count * tokens * depth * half * 2,
            bytes_accessed=count * depth * (tokens + 2 * half) * 2,
            transcendentals=0,
        ),
    )(which, *blocks, *halves, *extra)


def along_z(array):
    zs = lax.axis_size("z")
    pairs = [(c * zs + z, c * zs + (z + (1 - 2 * c)) % zs) for c in range(2) for z in range(zs)]
    return lax.ppermute(array, ("c", "z"), pairs)


def loss(hidden, weight, targets, domains, seq_len):
    core, z = lax.axis_index("c"), lax.axis_index("z")
    zs, ys = lax.axis_size("z"), lax.axis_size("y")
    halves = gathered_weight(weight)
    mine = to_all(hidden.T, "y", ys).reshape(BLOCK, -1).T
    rings = zs // 2
    own = [mine]
    other = [lax.ppermute(mine, "c", SWAP)]
    for r in range(1, rings + 1):
        own.append(along_z(own[-1]))
        if r < rings:
            other.append(along_z(other[-1]))
    swapped = []
    for some in BATCHES:
        swapped.append(lax.ppermute(jnp.stack([other[r] for r in some]), "c", SWAP))
    step = 2 * core - 1
    columns = weight.shape[1]
    half = columns // 2
    starts = jnp.stack([core * half, (1 - core) * half])
    wanted = (targets - lax.axis_index(VOCAB) * columns)[:, None]
    logits = None
    for name, rounds, batches in GROUPS:
        away = [r for r in rounds] + [-r for k in batches for r in BATCHES[k]]
        which = lax.rem(z + step * jnp.array(away, jnp.int32) + zs, zs)
        blocks = [own[r] for r in rounds] + [swapped[k] for k in batches]
        if name == "late":
            which = jnp.concatenate([which, starts])
            stats = product(which, blocks, halves, tuple(logits), wanted)
        else:
            logits = product(which, blocks, halves, logits and tuple(logits))
    return tail(stats[:2], domains, seq_len)


def solution(mesh):
    split = Mesh(mesh.devices.reshape(4, 2, 16, 4), ("x", "c", "z", "y"))
    placed = (P(TOK, VOCAB), P(TOK, VOCAB), P(TOK), P(TOK), P(TOK))
    return jax.shard_map(
        loss, mesh=split, in_specs=placed, out_specs=(P((*TOK, *VOCAB)), P()), check_vma=False
    )
```

```python
import jax
import jax.numpy as jnp
from jax import lax
from jax.experimental import pallas as pl
from jax.experimental.pallas import tpu as pltpu
from jax.sharding import Mesh
from jax.sharding import PartitionSpec as P


SEQ_LEN = 128
DOMAINS = 64
TOK = ("x", "c")
VOCAB = ("z", "y")
SWAP = [(0, 1), (1, 0)]
BLOCK = 256
TILE = 256
LONG = 512
LIMIT = 24 << 20
ROUNDS = 8
BATCHES = ((1, 2, 3), (4, 5, 6), (7,))
GROUPS = (
    ("early", range(0, 7), (0,)),
    ("middle", (7,), (1,)),
    ("late", (8,), (2,)),
)


def to_all(array, axis, copies):
    return lax.all_to_all(
        jnp.broadcast_to(array[None], (copies, *array.shape)), axis, 0, 0, tiled=True
    )


def gathered_weight(weight):
    own = to_all(weight, "x", lax.axis_size("x"))
    return own, lax.ppermute(own, "c", SWAP)


def tail(stats, domains, seq_len):
    tokens = stats.shape[1]
    zs, ys = lax.axis_size("z"), lax.axis_size("y")
    own = tokens // (zs * ys)
    y = lax.axis_index("y")
    slices = stats.reshape(2, zs, ys, own).transpose(2, 0, 1, 3)
    send = jnp.broadcast_to(slices.reshape(1, ys, -1), (zs, ys, 2 * zs * own))
    got = lax.all_to_all(send.reshape(zs * ys, -1), VOCAB, 0, 0, tiled=True)
    got = got.reshape(zs * ys, 2, zs * own)
    top = jnp.max(got[:, 0], axis=0)
    total = jnp.sum(jnp.exp(got[:, 0] - top[None]), axis=0)
    raw = jnp.log(total) + top - jnp.sum(got[:, 1], axis=0)
    index = lax.iota(jnp.int32, zs * own)
    local = (index // own) * (ys * own) + y * own + index % own
    seqs = seq_len.shape[0]
    lengths = jnp.sum(
        jnp.where((local // SEQ_LEN)[:, None] == lax.broadcasted_iota(jnp.int32, (zs * own, seqs), 1), seq_len[None], 0),
        axis=1,
    )
    mask = (local % SEQ_LEN < lengths).astype(jnp.float32)
    loss = raw * mask
    domain = lax.dynamic_index_in_dim(domains.reshape(zs, ys, own), y, 1, False).reshape(-1)
    here = domain[None, :] == lax.broadcasted_iota(jnp.int32, (DOMAINS, zs * own), 0)
    sums = jnp.sum(jnp.where(here, loss[None], 0.0), axis=1)
    counts = jnp.sum(jnp.where(here, mask[None], 0.0), axis=1)
    part = jnp.concatenate([sums, counts])
    axes = ("x", "c", "y")
    whole = jnp.sum(to_all(part, axes, lax.axis_size(axes)), axis=0)
    mean = whole[:DOMAINS] / jnp.maximum(whole[DOMAINS:], 1.0)
    token_loss = lax.dynamic_index_in_dim(loss.reshape(zs, own), lax.axis_index("z"), 0, False)
    return token_loss, mean


def product_kernel(kinds, first, last):
    def kernel(which, *refs):
        refs = list(refs)
        blocks = []
        for kind in kinds:
            if kind == "parts":
                blocks.append((refs.pop(0), refs.pop(0)))
            else:
                ref = refs.pop(0)
                blocks += [(ref.at[k],) for k in range(kind)] if kind else [(ref,)]
        count, weights = len(blocks), (refs.pop(0), refs.pop(0))
        before = None if first else refs.pop(0)
        wanted = refs.pop(0) if last else None
        out, rows, sems, *more = refs
        acc = more[0] if last else out

        def fetch(k, source):
            z = which[k]
            return pltpu.make_async_copy(
                source.at[z // 4, pl.ds((z % 2) * BLOCK, BLOCK)],
                rows.at[pl.ds(k * BLOCK, BLOCK)],
                sems.at[k],
            )

        for k in range(count):
            mine = (which[k] // 2) % 2 == which[count]
            pl.when(mine)(fetch(k, weights[0]).start)
            pl.when(jnp.logical_not(mine))(fetch(k, weights[1]).start)

        def tile(block, at):
            ref, at = (block[0], at) if len(block) == 1 or at < LONG else (block[1], at - LONG)
            return ref[at : at + TILE]

        tokens, columns = acc.shape
        steps = [range(0, min(2, count)), range(2, count)]
        steps = [ks for ks in steps if len(ks)]
        for n, ks in enumerate(steps):
            for k in ks:
                fetch(k, weights[0]).wait()
            deep = slice(ks[0] * BLOCK, (ks[-1] + 1) * BLOCK)
            for at in range(0, tokens, TILE):
                part = slice(at, at + TILE)
                left = jnp.concatenate([tile(blocks[k], at) for k in ks], axis=1)
                for low in range(0, columns, LONG):
                    side = slice(low, low + LONG)
                    total = jnp.dot(left, rows[deep, side], preferred_element_type=jnp.float32)
                    if n:
                        total += acc[part, side]
                    elif not first:
                        total += before[part, side]
                    acc[part, side] = total
                if last and n == len(steps) - 1:
                    values = acc[part]
                    top = jnp.max(values, axis=1, keepdims=True)
                    total = jnp.sum(jnp.exp(values - top), axis=1, keepdims=True)
                    lane = lax.broadcasted_iota(jnp.int32, values.shape, 1)
                    picked = jnp.where(lane == wanted[part], values, 0.0)
                    picked = jnp.sum(picked, axis=1, keepdims=True)
                    lse = jnp.log(total) + top
                    lane = lax.broadcasted_iota(jnp.int32, (TILE, 128), 1)
                    out[:, part] = jnp.where(lane == 0, lse, picked).T[:8]

    return kernel


def product(which, blocks, weights, before=None, wanted=None):
    kinds = ["parts" if isinstance(b, tuple) else b.shape[0] if b.ndim == 3 else 0 for b in blocks]
    count = sum(1 if kind == "parts" else kind or 1 for kind in kinds)
    arrays = [array for b in blocks for array in (b if isinstance(b, tuple) else (b,))]
    columns, tokens, last = weights[0].shape[2], 768, wanted is not None
    vmem = pl.BlockSpec(memory_space=pltpu.VMEM)
    extra = [array for array in (before, wanted) if array is not None]
    shape = (8, tokens) if last else (tokens, columns)
    return pl.pallas_call(
        product_kernel(kinds, before is None, last),
        in_specs=[pl.BlockSpec(memory_space=pltpu.SMEM)]
        + [vmem] * len(arrays)
        + [pl.BlockSpec(memory_space=pltpu.HBM)] * 2
        + [vmem] * len(extra),
        out_specs=vmem,
        out_shape=jax.ShapeDtypeStruct(shape, jnp.float32),
        scratch_shapes=[
            pltpu.VMEM((count * BLOCK, columns), jnp.bfloat16),
            pltpu.SemaphoreType.DMA((count,)),
        ]
        + ([pltpu.VMEM((tokens, columns), jnp.float32)] if last else []),
        input_output_aliases={} if before is None or last else {3 + len(arrays): 0},
        compiler_params=pltpu.CompilerParams(vmem_limit_bytes=LIMIT),
        cost_estimate=pl.CostEstimate(
            flops=2 * count * tokens * BLOCK * columns,
            bytes_accessed=count * BLOCK * (tokens + columns) * 2,
            transcendentals=0,
        ),
    )(which, *arrays, *weights, *extra)


def along_z(array):
    zs = lax.axis_size("z")
    pairs = [(c * zs + z, c * zs + (z + (1 - 2 * c)) % zs) for c in range(2) for z in range(zs)]
    return lax.ppermute(array, ("c", "z"), pairs)


def loss(hidden, weight, targets, domains, seq_len):
    core, z = lax.axis_index("c"), lax.axis_index("z")
    zs, ys = lax.axis_size("z"), lax.axis_size("y")
    weights = gathered_weight(weight)
    mine = to_all(hidden.T, "y", ys).reshape(BLOCK, -1).T
    theirs = lax.ppermute(mine, "c", SWAP)
    a, b = [mine[:LONG]], [jnp.concatenate([mine[LONG:], theirs[LONG:]], 0)]
    c = [theirs[:LONG]]
    for r in range(1, ROUNDS + 1):
        a.append(along_z(a[-1]))
        b.append(along_z(b[-1] if r < ROUNDS else b[-1][: mine.shape[0] - LONG]))
        if r < ROUNDS:
            c.append(along_z(c[-1]))
    swapped = []
    for some in BATCHES:
        give = [jnp.concatenate([c[r], b[r][mine.shape[0] - LONG :]], 0) for r in some]
        swapped.append(lax.ppermute(jnp.stack(give), "c", SWAP))
    step = 2 * core - 1
    wanted = (targets - lax.axis_index(VOCAB) * weight.shape[1])[:, None]
    logits = None
    for name, rounds, batches in GROUPS:
        away = [r for r in rounds] + [-r for k in batches for r in BATCHES[k]]
        which = lax.rem(z + step * jnp.array(away, jnp.int32) + zs, zs)
        which = jnp.concatenate([which, core[None]])
        blocks = [(a[r], b[r]) if r else mine for r in rounds] + [swapped[k] for k in batches]
        logits = product(which, blocks, weights, logits, wanted if name == "late" else None)
    return tail(logits[:2], domains, seq_len)


def solution(mesh):
    split = Mesh(mesh.devices.reshape(4, 2, 16, 4), ("x", "c", "z", "y"))
    placed = (P(TOK, VOCAB), P(TOK, VOCAB), P(TOK), P(TOK), P(TOK))
    return jax.shard_map(loss, mesh=split, in_specs=placed, out_specs=(P((*TOK, *VOCAB)), P()), check_vma=False)
```

```python
import jax
import jax.numpy as jnp
from jax import lax
from jax.experimental import pallas as pl
from jax.experimental.pallas import tpu as pltpu
from jax.sharding import Mesh
from jax.sharding import PartitionSpec as P


SEQ_LEN = 128
DOMAINS = 64
TOK = ("x", "c")
VOCAB = ("z", "y")
SWAP = [(0, 1), (1, 0)]
BLOCK = 256
TILE = 256
LONG = 512
LIMIT = 24 << 20
ROUNDS = 8
BATCHES = ((1, 2, 3), (4, 5, 6), (7,))
GROUPS = (
    ("early", range(0, 6), (0,)),
    ("middle", (6, 7), (1,)),
    ("late", (8,), (2,)),
)


def to_all(array, axis, copies):
    return lax.all_to_all(
        jnp.broadcast_to(array[None], (copies, *array.shape)), axis, 0, 0, tiled=True
    )


def gathered_weight(weight):
    own = to_all(weight, "x", lax.axis_size("x"))
    return own, lax.ppermute(own, "c", SWAP)


def tail(stats, domains, seq_len):
    tokens = stats.shape[1]
    zs, ys = lax.axis_size("z"), lax.axis_size("y")
    own = tokens // (zs * ys)
    y = lax.axis_index("y")
    slices = stats.reshape(2, zs, ys, own).transpose(2, 0, 1, 3)
    send = jnp.broadcast_to(slices.reshape(1, ys, -1), (zs, ys, 2 * zs * own))
    got = lax.all_to_all(send.reshape(zs * ys, -1), VOCAB, 0, 0, tiled=True)
    got = got.reshape(zs * ys, 2, zs * own)
    top = jnp.max(got[:, 0], axis=0)
    total = jnp.sum(jnp.exp(got[:, 0] - top[None]), axis=0)
    raw = jnp.log(total) + top - jnp.sum(got[:, 1], axis=0)
    index = lax.iota(jnp.int32, zs * own)
    local = (index // own) * (ys * own) + y * own + index % own
    seqs = seq_len.shape[0]
    lengths = jnp.sum(
        jnp.where((local // SEQ_LEN)[:, None] == lax.broadcasted_iota(jnp.int32, (zs * own, seqs), 1), seq_len[None], 0),
        axis=1,
    )
    mask = (local % SEQ_LEN < lengths).astype(jnp.float32)
    loss = raw * mask
    domain = lax.dynamic_index_in_dim(domains.reshape(zs, ys, own), y, 1, False).reshape(-1)
    here = domain[None, :] == lax.broadcasted_iota(jnp.int32, (DOMAINS, zs * own), 0)
    sums = jnp.sum(jnp.where(here, loss[None], 0.0), axis=1)
    counts = jnp.sum(jnp.where(here, mask[None], 0.0), axis=1)
    part = jnp.concatenate([sums, counts])
    axes = ("x", "c", "y")
    whole = jnp.sum(to_all(part, axes, lax.axis_size(axes)), axis=0)
    mean = whole[:DOMAINS] / jnp.maximum(whole[DOMAINS:], 1.0)
    token_loss = lax.dynamic_index_in_dim(loss.reshape(zs, own), lax.axis_index("z"), 0, False)
    return token_loss, mean


def product_kernel(kinds, first, last):
    def kernel(which, *refs):
        refs = list(refs)
        blocks = []
        for kind in kinds:
            if kind == "parts":
                blocks.append((refs.pop(0), refs.pop(0)))
            else:
                ref = refs.pop(0)
                blocks += [(ref.at[k],) for k in range(kind)] if kind else [(ref,)]
        count, weights = len(blocks), (refs.pop(0), refs.pop(0))
        before = None if first else refs.pop(0)
        wanted = refs.pop(0) if last else None
        out, rows, sems, *more = refs
        acc = more[0] if last else out

        def fetch(k, source):
            z = which[k]
            return pltpu.make_async_copy(
                source.at[z // 4, pl.ds((z % 2) * BLOCK, BLOCK)],
                rows.at[pl.ds(k * BLOCK, BLOCK)],
                sems.at[k],
            )

        for k in range(count):
            mine = (which[k] // 2) % 2 == which[count]
            pl.when(mine)(fetch(k, weights[0]).start)
            pl.when(jnp.logical_not(mine))(fetch(k, weights[1]).start)

        def tile(block, at):
            ref, at = (block[0], at) if len(block) == 1 or at < LONG else (block[1], at - LONG)
            return ref[at : at + TILE]

        tokens, columns = acc.shape
        steps = [range(0, min(2, count)), range(2, count)]
        steps = [ks for ks in steps if len(ks)]
        for n, ks in enumerate(steps):
            for k in ks:
                fetch(k, weights[0]).wait()
            deep = slice(ks[0] * BLOCK, (ks[-1] + 1) * BLOCK)
            for at in range(0, tokens, TILE):
                part = slice(at, at + TILE)
                left = jnp.concatenate([tile(blocks[k], at) for k in ks], axis=1)
                for low in range(0, columns, LONG):
                    side = slice(low, low + LONG)
                    total = jnp.dot(left, rows[deep, side], preferred_element_type=jnp.float32)
                    if n:
                        total += acc[part, side]
                    elif not first:
                        total += before[part, side]
                    acc[part, side] = total
                if last and n == len(steps) - 1:
                    values = acc[part]
                    top = jnp.max(values, axis=1, keepdims=True)
                    total = jnp.sum(jnp.exp(values - top), axis=1, keepdims=True)
                    lane = lax.broadcasted_iota(jnp.int32, values.shape, 1)
                    picked = jnp.where(lane == wanted[part], values, 0.0)
                    picked = jnp.sum(picked, axis=1, keepdims=True)
                    lse = jnp.log(total) + top
                    lane = lax.broadcasted_iota(jnp.int32, (TILE, 128), 1)
                    out[:, part] = jnp.where(lane == 0, lse, picked).T[:8]

    return kernel


def product(which, blocks, weights, before=None, wanted=None):
    kinds = ["parts" if isinstance(b, tuple) else b.shape[0] if b.ndim == 3 else 0 for b in blocks]
    count = sum(1 if kind == "parts" else kind or 1 for kind in kinds)
    arrays = [array for b in blocks for array in (b if isinstance(b, tuple) else (b,))]
    columns, tokens, last = weights[0].shape[2], 768, wanted is not None
    vmem = pl.BlockSpec(memory_space=pltpu.VMEM)
    extra = [array for array in (before, wanted) if array is not None]
    shape = (8, tokens) if last else (tokens, columns)
    return pl.pallas_call(
        product_kernel(kinds, before is None, last),
        in_specs=[pl.BlockSpec(memory_space=pltpu.SMEM)]
        + [vmem] * len(arrays)
        + [pl.BlockSpec(memory_space=pltpu.HBM)] * 2
        + [vmem] * len(extra),
        out_specs=vmem,
        out_shape=jax.ShapeDtypeStruct(shape, jnp.float32),
        scratch_shapes=[
            pltpu.VMEM((count * BLOCK, columns), jnp.bfloat16),
            pltpu.SemaphoreType.DMA((count,)),
        ]
        + ([pltpu.VMEM((tokens, columns), jnp.float32)] if last else []),
        input_output_aliases={} if before is None or last else {3 + len(arrays): 0},
        compiler_params=pltpu.CompilerParams(vmem_limit_bytes=LIMIT),
        cost_estimate=pl.CostEstimate(
            flops=2 * count * tokens * BLOCK * columns,
            bytes_accessed=count * BLOCK * (tokens + columns) * 2,
            transcendentals=0,
        ),
    )(which, *arrays, *weights, *extra)


def along_z(array):
    zs = lax.axis_size("z")
    pairs = [(c * zs + z, c * zs + (z + (1 - 2 * c)) % zs) for c in range(2) for z in range(zs)]
    return lax.ppermute(array, ("c", "z"), pairs)


def loss(hidden, weight, targets, domains, seq_len):
    core, z = lax.axis_index("c"), lax.axis_index("z")
    zs, ys = lax.axis_size("z"), lax.axis_size("y")
    weights = gathered_weight(weight)
    mine = to_all(hidden.T, "y", ys).reshape(BLOCK, -1).T
    theirs = lax.ppermute(mine, "c", SWAP)
    own, other = [mine], [theirs]
    for r in range(1, ROUNDS + 1):
        own.append(along_z(own[-1]))
        if r < ROUNDS:
            other.append(along_z(other[-1]))
    swapped = []
    for some in BATCHES:
        swapped.append(lax.ppermute(jnp.stack([other[r] for r in some]), "c", SWAP))
    step = 2 * core - 1
    wanted = (targets - lax.axis_index(VOCAB) * weight.shape[1])[:, None]
    logits = None
    for name, rounds, batches in GROUPS:
        away = [r for r in rounds] + [-r for k in batches for r in BATCHES[k]]
        which = lax.rem(z + step * jnp.array(away, jnp.int32) + zs, zs)
        which = jnp.concatenate([which, core[None]])
        blocks = [own[r] for r in rounds] + [swapped[k] for k in batches]
        logits = product(which, blocks, weights, logits, wanted if name == "late" else None)
    return tail(logits[:2], domains, seq_len)


def solution(mesh):
    split = Mesh(mesh.devices.reshape(4, 2, 16, 4), ("x", "c", "z", "y"))
    placed = (P(TOK, VOCAB), P(TOK, VOCAB), P(TOK), P(TOK), P(TOK))
    return jax.shard_map(loss, mesh=split, in_specs=placed, out_specs=(P((*TOK, *VOCAB)), P()), check_vma=False)
```

```python
import jax
import jax.numpy as jnp
from jax import lax
from jax.experimental import pallas as pl
from jax.experimental.pallas import tpu as pltpu
from jax.sharding import Mesh
from jax.sharding import PartitionSpec as P


SEQ_LEN = 128
DOMAINS = 64
TOK = ("x", "c")
VOCAB = ("z", "y")
SWAP = [(0, 1), (1, 0)]
BLOCK = 256
TILE = 256
LONG = 512
LIMIT = 60 << 20
ROUNDS = 8
BATCHES = ((1, 2, 3), (4, 5), (6, 7))
GROUPS = (
    ("early", range(0, 5), ()),
    ("middle", (5, 6, 7), (0, 1)),
    ("late", (8,), (2,)),
)


def to_all(array, axis, copies):
    return lax.all_to_all(
        jnp.broadcast_to(array[None], (copies, *array.shape)), axis, 0, 0, tiled=True
    )


def gathered_weight(weight):
    own = to_all(weight, "x", lax.axis_size("x"))
    return own, lax.ppermute(own, "c", SWAP)


def tail(stats, domains, seq_len):
    tokens = stats.shape[1]
    zs, ys = lax.axis_size("z"), lax.axis_size("y")
    own = tokens // (zs * ys)
    y = lax.axis_index("y")
    slices = stats.reshape(2, zs, ys, own).transpose(2, 0, 1, 3)
    send = jnp.broadcast_to(slices.reshape(1, ys, -1), (zs, ys, 2 * zs * own))
    got = lax.all_to_all(send.reshape(zs * ys, -1), VOCAB, 0, 0, tiled=True)
    got = got.reshape(zs * ys, 2, zs * own)
    top = jnp.max(got[:, 0], axis=0)
    total = jnp.sum(jnp.exp(got[:, 0] - top[None]), axis=0)
    raw = jnp.log(total) + top - jnp.sum(got[:, 1], axis=0)
    index = lax.iota(jnp.int32, zs * own)
    local = (index // own) * (ys * own) + y * own + index % own
    seqs = seq_len.shape[0]
    lengths = jnp.sum(
        jnp.where((local // SEQ_LEN)[:, None] == lax.broadcasted_iota(jnp.int32, (zs * own, seqs), 1), seq_len[None], 0),
        axis=1,
    )
    mask = (local % SEQ_LEN < lengths).astype(jnp.float32)
    loss = raw * mask
    domain = lax.dynamic_index_in_dim(domains.reshape(zs, ys, own), y, 1, False).reshape(-1)
    here = domain[None, :] == lax.broadcasted_iota(jnp.int32, (DOMAINS, zs * own), 0)
    sums = jnp.sum(jnp.where(here, loss[None], 0.0), axis=1)
    counts = jnp.sum(jnp.where(here, mask[None], 0.0), axis=1)
    part = jnp.concatenate([sums, counts])
    axes = ("x", "c", "y")
    whole = jnp.sum(to_all(part, axes, lax.axis_size(axes)), axis=0)
    mean = whole[:DOMAINS] / jnp.maximum(whole[DOMAINS:], 1.0)
    token_loss = lax.dynamic_index_in_dim(loss.reshape(zs, own), lax.axis_index("z"), 0, False)
    return token_loss, mean


def product_kernel(kinds, first, last):
    def kernel(which, *refs):
        refs = list(refs)
        blocks = []
        for kind in kinds:
            ref = refs.pop(0)
            blocks += [ref.at[k] for k in range(kind)] if kind else [ref]
        count, weights = len(blocks), (refs.pop(0), refs.pop(0))
        before = None if first else refs.pop(0)
        wanted = refs.pop(0) if last else None
        out, acc, rows, lefts, sems, ends = refs

        def fetch(k, source):
            z = which[k]
            return pltpu.make_async_copy(
                source.at[z // 4, pl.ds((z % 2) * BLOCK, BLOCK)],
                rows.at[pl.ds(k * BLOCK, BLOCK)],
                sems.at[0, k],
            )

        def fetch_block(k):
            return pltpu.make_async_copy(blocks[k], lefts.at[k], sems.at[1, k])

        def whole(part, source, target, n):
            return pltpu.make_async_copy(source.at[part], target.at[part], ends.at[n])

        tokens, columns = acc.shape
        parts = [slice(at, at + TILE) for at in range(0, tokens, TILE)]
        for k in range(count):
            fetch_block(k).start()
            mine = (which[k] // 2) % 2 == which[count]
            pl.when(mine)(fetch(k, weights[0]).start)
            pl.when(jnp.logical_not(mine))(fetch(k, weights[1]).start)

        if not first:
            for n, part in enumerate(parts):
                whole(part, before, acc, n).start()
        steps = [range(0, min(2, count)), range(2, count)]
        steps = [ks for ks in steps if len(ks)]
        for n, ks in enumerate(steps):
            for k in ks:
                fetch_block(k).wait()
                fetch(k, weights[0]).wait()
            deep = slice(ks[0] * BLOCK, (ks[-1] + 1) * BLOCK)
            for place, part in enumerate(parts):
                left = jnp.concatenate([lefts[k, part] for k in ks], axis=1)
                if n == 0 and not first:
                    whole(part, before, acc, place).wait()
                for low in range(0, columns, LONG):
                    side = slice(low, low + LONG)
                    total = jnp.dot(left, rows[deep, side], preferred_element_type=jnp.float32)
                    acc[part, side] = total if n == 0 and first else total + acc[part, side]
                if n < len(steps) - 1:
                    continue
                if not last:
                    whole(part, acc, out, place).start()
                else:
                    values = acc[part]
                    top = jnp.max(values, axis=1, keepdims=True)
                    total = jnp.sum(jnp.exp(values - top), axis=1, keepdims=True)
                    lane = lax.broadcasted_iota(jnp.int32, values.shape, 1)
                    picked = jnp.where(lane == wanted[part], values, 0.0)
                    picked = jnp.sum(picked, axis=1, keepdims=True)
                    lse = jnp.log(total) + top
                    lane = lax.broadcasted_iota(jnp.int32, (TILE, 128), 1)
                    out[:, part] = jnp.where(lane == 0, lse, picked).T[:8]
        if not last:
            for place, part in enumerate(parts):
                whole(part, acc, out, place).wait()

    return kernel


def product(which, blocks, weights, before=None, wanted=None):
    kinds = [b.shape[0] if b.ndim == 3 else 0 for b in blocks]
    count = sum(kind or 1 for kind in kinds)
    columns, tokens, last = weights[0].shape[2], 768, wanted is not None
    vmem = pl.BlockSpec(memory_space=pltpu.VMEM)
    hbm = pl.BlockSpec(memory_space=pltpu.HBM)
    shape = (8, tokens) if last else (tokens, columns)
    return pl.pallas_call(
        product_kernel(kinds, before is None, last),
        in_specs=[pl.BlockSpec(memory_space=pltpu.SMEM)]
        + [hbm] * (len(blocks) + 2)
        + [hbm] * (before is not None)
        + [vmem] * last,
        out_specs=vmem if last else hbm,
        out_shape=jax.ShapeDtypeStruct(shape, jnp.float32),
        scratch_shapes=[
            pltpu.VMEM((tokens, columns), jnp.float32),
            pltpu.VMEM((count * BLOCK, columns), jnp.bfloat16),
            pltpu.VMEM((count, tokens, BLOCK), jnp.bfloat16),
            pltpu.SemaphoreType.DMA((2, count)),
            pltpu.SemaphoreType.DMA((tokens // TILE,)),
        ],
        compiler_params=pltpu.CompilerParams(vmem_limit_bytes=LIMIT),
        cost_estimate=pl.CostEstimate(
            flops=2 * count * tokens * BLOCK * columns,
            bytes_accessed=count * BLOCK * (tokens + columns) * 2,
            transcendentals=0,
        ),
    )(which, *blocks, *weights, *(array for array in (before, wanted) if array is not None))


def along_z(array):
    zs = lax.axis_size("z")
    pairs = [(c * zs + z, c * zs + (z + (1 - 2 * c)) % zs) for c in range(2) for z in range(zs)]
    return lax.ppermute(array, ("c", "z"), pairs)


def loss(hidden, weight, targets, domains, seq_len):
    core, z = lax.axis_index("c"), lax.axis_index("z")
    zs, ys = lax.axis_size("z"), lax.axis_size("y")
    weights = gathered_weight(weight)
    mine = to_all(hidden.T, "y", ys).reshape(BLOCK, -1).T
    theirs = lax.ppermute(mine, "c", SWAP)
    own, other = [mine], [theirs]
    for r in range(1, ROUNDS + 1):
        own.append(along_z(own[-1]))
        if r < ROUNDS:
            other.append(along_z(other[-1]))
    swapped = []
    for some in BATCHES:
        swapped.append(lax.ppermute(jnp.stack([other[r] for r in some]), "c", SWAP))
    step = 2 * core - 1
    wanted = (targets - lax.axis_index(VOCAB) * weight.shape[1])[:, None]
    logits = None
    for name, rounds, batches in GROUPS:
        away = [r for r in rounds] + [-r for k in batches for r in BATCHES[k]]
        which = lax.rem(z + step * jnp.array(away, jnp.int32) + zs, zs)
        which = jnp.concatenate([which, core[None]])
        blocks = [own[r] for r in rounds] + [swapped[k] for k in batches]
        logits = product(which, blocks, weights, logits, wanted if name == "late" else None)
    return tail(logits[:2], domains, seq_len)


def solution(mesh):
    split = Mesh(mesh.devices.reshape(4, 2, 16, 4), ("x", "c", "z", "y"))
    placed = (P(TOK, VOCAB), P(TOK, VOCAB), P(TOK), P(TOK), P(TOK))
    return jax.shard_map(loss, mesh=split, in_specs=placed, out_specs=(P((*TOK, *VOCAB)), P()), check_vma=False)
```

```python
import jax
import jax.numpy as jnp
from jax import lax
from jax.experimental import pallas as pl
from jax.experimental.pallas import tpu as pltpu
from jax.sharding import Mesh
from jax.sharding import PartitionSpec as P


SEQ_LEN = 128
DOMAINS = 64
TOK = ("x", "c")
VOCAB = ("z", "y")
SWAP = [(0, 1), (1, 0)]
BLOCK = 256
TILE = 256
LONG = 512
LIMIT = 60 << 20
ROUNDS = 8
BATCHES = ((1, 2, 3), (4, 5, 6), (7,))
DEPTHS = (0, 2, 6, 11, 16)


def to_all(array, axis, copies):
    return lax.all_to_all(
        jnp.broadcast_to(array[None], (copies, *array.shape)), axis, 0, 0, tiled=True
    )


def along_z(array):
    zs = lax.axis_size("z")
    pairs = [(c * zs + z, c * zs + (z + (1 - 2 * c)) % zs) for c in range(2) for z in range(zs)]
    return lax.ppermute(array, ("c", "z"), pairs)


def gathered_weight(weight):
    own = to_all(weight, "x", lax.axis_size("x"))
    return own, lax.ppermute(own, "c", SWAP)


def before_tail(tokens, z, y, domains, seq_len):
    zs, ys = lax.axis_size("z"), lax.axis_size("y")
    own = tokens // (zs * ys)
    index = lax.iota(jnp.int32, zs * own)
    local = (index // own) * (ys * own) + y * own + index % own
    sequence = lax.broadcasted_iota(jnp.int32, (zs * own, seq_len.shape[0]), 1)
    of_token = (local // SEQ_LEN)[:, None] == sequence
    lengths = jnp.sum(jnp.where(of_token, seq_len[None], 0), axis=1)
    mask = (local % SEQ_LEN < lengths).astype(jnp.float32)
    place = lax.broadcasted_iota(jnp.int32, (zs, ys, own), 1)
    domain = jnp.sum(jnp.where(place == y, domains.reshape(zs, ys, own), 0), axis=1).reshape(-1)
    here = domain[None, :] == lax.broadcasted_iota(jnp.int32, (DOMAINS, zs * own), 0)
    here = here.astype(jnp.float32)
    outputs = (lax.broadcasted_iota(jnp.int32, (zs, own), 0) == z).astype(jnp.float32)
    return mask, here, outputs, jnp.sum(here * mask[None], axis=1)


def tail(stats, mask, here, outputs, counts):
    zs, ys = lax.axis_size("z"), lax.axis_size("y")
    own = stats.shape[1] // (zs * ys)
    slices = stats.reshape(2, zs, ys, own).transpose(2, 0, 1, 3)
    send = jnp.broadcast_to(slices.reshape(1, ys, -1), (zs, ys, 2 * zs * own))
    got = lax.all_to_all(send.reshape(zs * ys, -1), VOCAB, 0, 0, tiled=True)
    got = got.reshape(zs * ys, 2, zs * own)
    top = jnp.max(got[:, 0], axis=0)
    total = jnp.sum(jnp.exp(got[:, 0] - top[None]), axis=0)
    loss = (jnp.log(total) + top - jnp.sum(got[:, 1], axis=0)) * mask
    sums = jnp.sum(jnp.where(here > 0, loss[None], 0.0), axis=1)
    token_loss = jnp.sum(jnp.where(outputs > 0, loss.reshape(zs, own), 0.0), axis=0)
    part, token_loss = lax.optimization_barrier((jnp.concatenate([sums, counts]), token_loss))
    axes = ("x", "c", "y")
    whole = jnp.sum(to_all(part, axes, lax.axis_size(axes)), axis=0)
    mean = whole[:DOMAINS] / jnp.maximum(whole[DOMAINS:], 1.0)
    return token_loss, mean


def product_kernel(kinds, away):
    def kernel(where, *refs):
        refs = list(refs)
        blocks = []
        for kind in kinds:
            ref = refs.pop(0)
            blocks += [ref.at[k] for k in range(kind)] if kind else [ref]
        own, theirs, wanted, out, acc, rows, lefts, sems = refs
        core, z = where[0], where[1]

        def fetch(k, weights, source):
            return pltpu.make_async_copy(
                weights.at[source // 4, pl.ds(lax.rem(source, 2) * BLOCK, BLOCK)],
                rows.at[pl.ds(k * BLOCK, BLOCK)],
                sems.at[0, k],
            )

        def fetch_block(k):
            return pltpu.make_async_copy(blocks[k], lefts.at[k], sems.at[1, k])

        for k, far in enumerate(away):
            source = lax.rem(z + far * (2 * core - 1) + 16, 16)
            fetch_block(k).start()
            mine = lax.rem(source // 2, 2) == core
            pl.when(mine)(fetch(k, own, source).start)
            pl.when(jnp.logical_not(mine))(fetch(k, theirs, source).start)

        tokens, columns = acc.shape
        for first, end in zip(DEPTHS, DEPTHS[1:]):
            for k in range(first, end):
                fetch_block(k).wait()
                fetch(k, own, 0).wait()
            deep = slice(first * BLOCK, end * BLOCK)
            for at in range(0, tokens, TILE):
                part = slice(at, at + TILE)
                left = jnp.concatenate([lefts[k, part] for k in range(first, end)], axis=1)
                for begin in range(0, columns, LONG):
                    side = slice(begin, begin + LONG)
                    total = jnp.dot(left, rows[deep, side], preferred_element_type=jnp.float32)
                    acc[part, side] = total + acc[part, side] if first else total
                if end < len(away):
                    continue
                values = acc[part]
                top = jnp.max(values, axis=1, keepdims=True)
                total = jnp.sum(jnp.exp(values - top), axis=1, keepdims=True)
                lane = lax.broadcasted_iota(jnp.int32, values.shape, 1)
                picked = jnp.where(lane == wanted[part], values, 0.0)
                picked = jnp.sum(picked, axis=1, keepdims=True)
                lse = jnp.log(total) + top
                lane = lax.broadcasted_iota(jnp.int32, (TILE, 128), 1)
                out[:, part] = jnp.where(lane == 0, lse, picked).T[:8]

    return kernel


def product(where, away, blocks, weights, wanted):
    kinds = [b.shape[0] if b.ndim == 3 else 0 for b in blocks]
    count, tokens, columns = len(away), blocks[0].shape[-2], weights[0].shape[2]
    vmem = pl.BlockSpec(memory_space=pltpu.VMEM)
    hbm = pl.BlockSpec(memory_space=pltpu.HBM)
    return pl.pallas_call(
        product_kernel(kinds, away),
        in_specs=[pl.BlockSpec(memory_space=pltpu.SMEM)] + [hbm] * (len(blocks) + 2) + [vmem],
        out_specs=vmem,
        out_shape=jax.ShapeDtypeStruct((8, tokens), jnp.float32),
        scratch_shapes=[
            pltpu.VMEM((tokens, columns), jnp.float32),
            pltpu.VMEM((count * BLOCK, columns), jnp.bfloat16),
            pltpu.VMEM((count, tokens, BLOCK), jnp.bfloat16),
            pltpu.SemaphoreType.DMA((2, count)),
        ],
        compiler_params=pltpu.CompilerParams(vmem_limit_bytes=LIMIT),
        cost_estimate=pl.CostEstimate(
            flops=2 * count * tokens * BLOCK * columns,
            bytes_accessed=count * BLOCK * (tokens + columns) * 2,
            transcendentals=tokens * columns,
        ),
    )(where, *blocks, *weights, wanted)


def loss(hidden, weight, targets, domains, seq_len):
    ys = lax.axis_size("y")
    core, z, y = (lax.axis_index(name) for name in ("c", "z", "y"))
    low = lax.axis_index(VOCAB) * weight.shape[1]
    hidden, where, z, y, low = lax.optimization_barrier((hidden, jnp.stack([core, z]), z, y, low))
    mine = to_all(hidden.T, "y", ys).reshape(BLOCK, -1).T
    theirs = lax.ppermute(mine, "c", SWAP)
    weights = gathered_weight(weight)
    own, other = [mine], [theirs]
    for r in range(1, ROUNDS + 1):
        own.append(along_z(own[-1]))
        if r == 2:
            domains, seq_len, targets, own[2] = lax.optimization_barrier(
                (domains, seq_len, targets, own[2])
            )
            ready = before_tail(targets.shape[0], z, y, domains, seq_len)
            wanted = (targets - low)[:, None]
        if r == 4:
            own[4], ready, wanted = lax.optimization_barrier((own[4], ready, wanted))
        if r < ROUNDS:
            other.append(along_z(other[-1]))
    swapped = []
    for some in BATCHES:
        swapped.append(lax.ppermute(jnp.stack([other[r] for r in some]), "c", SWAP))
    away = [*range(7), *(-r for some in BATCHES[:2] for r in some), 7, 8, *(-r for r in BATCHES[2])]
    blocks = [*own[:7], *swapped[:2], own[7], own[8], swapped[2]]
    stats = product(where, away, blocks, weights, wanted)
    return tail(stats[:2], *ready)


def solution(mesh):
    split = Mesh(mesh.devices.reshape(4, 2, 16, 4), ("x", "c", "z", "y"))
    placed = (P(TOK, VOCAB), P(TOK, VOCAB), P(TOK), P(TOK), P(TOK))
    return jax.shard_map(loss, mesh=split, in_specs=placed, out_specs=(P((*TOK, *VOCAB)), P()), check_vma=False)
```

```python
import jax
import jax.numpy as jnp
from jax import lax
from jax.experimental import pallas as pl
from jax.experimental.pallas import tpu as pltpu
from jax.sharding import Mesh
from jax.sharding import PartitionSpec as P


SEQ_LEN = 128
DOMAINS = 64
TOK = ("x", "c")
VOCAB = ("z", "y")
SWAP = [(0, 1), (1, 0)]
BLOCK = 256
TILE = 256
LONG = 512
LIMIT = 60 << 20
ROUNDS = 8
BATCHES = ((1, 2, 3), (4, 5, 6), (7,))
DEPTHS = (0, 2, 6, 11, 16)


def to_all(array, axis, copies):
    return lax.all_to_all(
        jnp.broadcast_to(array[None], (copies, *array.shape)), axis, 0, 0, tiled=True
    )


def along(array, axis, step, core_step=0):
    size = lax.axis_size(axis)
    way = [step + core_step * c for c in range(2)]
    if axis == "z":
        pairs = [(c * size + i, c * size + (i + way[c]) % size) for c in range(2) for i in range(size)]
        return lax.ppermute(array, ("c", "z"), pairs)
    pairs = [(2 * i + c, 2 * ((i + way[c]) % size) + c) for c in range(2) for i in range(size)]
    return lax.ppermute(array, TOK, pairs)


def along_z(array):
    return along(array, "z", 1, -2)


def gathered_weight(weight, core):
    third = along(weight, "x", 1)
    first = along(weight, "x", -1)
    second = along(jnp.where(core == 0, third, first), "x", 1, -2)
    own = [weight, first, second, third]
    theirs = []
    for shard in own:
        theirs.append(lax.ppermute(shard, "c", SWAP))
    return own + theirs


def before_tail(tokens, z, y, domains, seq_len):
    zs, ys = lax.axis_size("z"), lax.axis_size("y")
    own = tokens // (zs * ys)
    index = lax.iota(jnp.int32, zs * own)
    local = (index // own) * (ys * own) + y * own + index % own
    sequence = lax.broadcasted_iota(jnp.int32, (zs * own, seq_len.shape[0]), 1)
    of_token = (local // SEQ_LEN)[:, None] == sequence
    lengths = jnp.sum(jnp.where(of_token, seq_len[None], 0), axis=1)
    mask = (local % SEQ_LEN < lengths).astype(jnp.float32)
    place = lax.broadcasted_iota(jnp.int32, (zs, ys, own), 1)
    domain = jnp.sum(jnp.where(place == y, domains.reshape(zs, ys, own), 0), axis=1).reshape(-1)
    here = domain[None, :] == lax.broadcasted_iota(jnp.int32, (DOMAINS, zs * own), 0)
    here = here.astype(jnp.float32)
    outputs = (lax.broadcasted_iota(jnp.int32, (zs, own), 0) == z).astype(jnp.float32)
    return mask, here, outputs, jnp.sum(here * mask[None], axis=1)


def tail(stats, mask, here, outputs, counts):
    zs, ys = lax.axis_size("z"), lax.axis_size("y")
    own = stats.shape[1] // (zs * ys)
    slices = stats.reshape(2, zs, ys, own).transpose(2, 0, 1, 3)
    send = jnp.broadcast_to(slices.reshape(1, ys, -1), (zs, ys, 2 * zs * own))
    got = lax.all_to_all(send.reshape(zs * ys, -1), VOCAB, 0, 0, tiled=True)
    got = got.reshape(zs * ys, 2, zs * own)
    top = jnp.max(got[:, 0], axis=0)
    total = jnp.sum(jnp.exp(got[:, 0] - top[None]), axis=0)
    loss = (jnp.log(total) + top - jnp.sum(got[:, 1], axis=0)) * mask
    sums = jnp.sum(jnp.where(here > 0, loss[None], 0.0), axis=1)
    token_loss = jnp.sum(jnp.where(outputs > 0, loss.reshape(zs, own), 0.0), axis=0)
    part, token_loss = lax.optimization_barrier((jnp.concatenate([sums, counts]), token_loss))
    axes = ("x", "c", "y")
    whole = jnp.sum(to_all(part, axes, lax.axis_size(axes)), axis=0)
    mean = whole[:DOMAINS] / jnp.maximum(whole[DOMAINS:], 1.0)
    return token_loss, mean


def product_kernel(kinds, away):
    def kernel(where, *refs):
        refs = list(refs)
        blocks = []
        for kind in kinds:
            ref = refs.pop(0)
            blocks += [ref.at[k] for k in range(kind)] if kind else [ref]
        *weights, wanted, out, acc, rows, lefts, sems = refs
        x, core, z = where[0], where[1], where[2]

        def fetch(k, weight, low):
            return pltpu.make_async_copy(
                weight.at[pl.ds(low, BLOCK)], rows.at[pl.ds(k * BLOCK, BLOCK)], sems.at[0, k]
            )

        def fetch_block(k):
            return pltpu.make_async_copy(blocks[k], lefts.at[k], sems.at[1, k])

        for k, far in enumerate(away):
            source = lax.rem(z + far * (2 * core - 1) + 16, 16)
            fetch_block(k).start()
            shard = lax.rem(source // 4 - x + 4, 4)
            shard += 4 * (lax.rem(source // 2, 2) != core).astype(jnp.int32)
            low = pl.multiple_of(lax.rem(source, 2) * BLOCK, BLOCK)
            for n, weight in enumerate(weights):
                pl.when(shard == n)(fetch(k, weight, low).start)

        tokens, columns = acc.shape
        for first, end in zip(DEPTHS, DEPTHS[1:]):
            for k in range(first, end):
                fetch_block(k).wait()
                fetch(k, weights[0], 0).wait()
            deep = slice(first * BLOCK, end * BLOCK)
            for at in range(0, tokens, TILE):
                part = slice(at, at + TILE)
                left = jnp.concatenate([lefts[k, part] for k in range(first, end)], axis=1)
                for begin in range(0, columns, LONG):
                    side = slice(begin, begin + LONG)
                    total = jnp.dot(left, rows[deep, side], preferred_element_type=jnp.float32)
                    acc[part, side] = total + acc[part, side] if first else total
                if end < len(away):
                    continue
                values = acc[part]
                top = jnp.max(values, axis=1, keepdims=True)
                total = jnp.sum(jnp.exp(values - top), axis=1, keepdims=True)
                lane = lax.broadcasted_iota(jnp.int32, values.shape, 1)
                picked = jnp.where(lane == wanted[part], values, 0.0)
                picked = jnp.sum(picked, axis=1, keepdims=True)
                lse = jnp.log(total) + top
                lane = lax.broadcasted_iota(jnp.int32, (TILE, 128), 1)
                out[:, part] = jnp.where(lane == 0, lse, picked).T[:8]

    return kernel


def product(where, away, blocks, weights, wanted):
    kinds = [b.shape[0] if b.ndim == 3 else 0 for b in blocks]
    count, tokens, columns = len(away), blocks[0].shape[-2], weights[0].shape[1]
    vmem = pl.BlockSpec(memory_space=pltpu.VMEM)
    hbm = pl.BlockSpec(memory_space=pltpu.HBM)
    return pl.pallas_call(
        product_kernel(kinds, away),
        in_specs=[pl.BlockSpec(memory_space=pltpu.SMEM)] + [hbm] * (len(blocks) + len(weights)) + [vmem],
        out_specs=vmem,
        out_shape=jax.ShapeDtypeStruct((8, tokens), jnp.float32),
        scratch_shapes=[
            pltpu.VMEM((tokens, columns), jnp.float32),
            pltpu.VMEM((count * BLOCK, columns), jnp.bfloat16),
            pltpu.VMEM((count, tokens, BLOCK), jnp.bfloat16),
            pltpu.SemaphoreType.DMA((2, count)),
        ],
        compiler_params=pltpu.CompilerParams(vmem_limit_bytes=LIMIT),
        cost_estimate=pl.CostEstimate(
            flops=2 * count * tokens * BLOCK * columns,
            bytes_accessed=count * BLOCK * (tokens + columns) * 2,
            transcendentals=tokens * columns,
        ),
    )(where, *blocks, *weights, wanted)


def loss(hidden, weight, targets, domains, seq_len):
    ys = lax.axis_size("y")
    x, core, z, y = (lax.axis_index(name) for name in ("x", "c", "z", "y"))
    low = lax.axis_index(VOCAB) * weight.shape[1]
    hidden, where, core, z, y, low = lax.optimization_barrier(
        (hidden, jnp.stack([x, core, z]), core, z, y, low)
    )
    mine = to_all(hidden.T, "y", ys).reshape(BLOCK, -1).T
    theirs = lax.ppermute(mine, "c", SWAP)
    weights = gathered_weight(weight, core)
    own, other = [mine], [theirs]
    for r in range(1, ROUNDS + 1):
        own.append(along_z(own[-1]))
        if r == 2:
            domains, seq_len, targets, own[2] = lax.optimization_barrier(
                (domains, seq_len, targets, own[2])
            )
            ready = before_tail(targets.shape[0], z, y, domains, seq_len)
            wanted = (targets - low)[:, None]
        if r == 4:
            own[4], ready, wanted = lax.optimization_barrier((own[4], ready, wanted))
        if r < ROUNDS:
            other.append(along_z(other[-1]))
    swapped = []
    for some in BATCHES:
        swapped.append(lax.ppermute(jnp.stack([other[r] for r in some]), "c", SWAP))
    away = [*range(7), *(-r for some in BATCHES[:2] for r in some), 7, 8, *(-r for r in BATCHES[2])]
    blocks = [*own[:7], *swapped[:2], own[7], own[8], swapped[2]]
    stats = product(where, away, blocks, weights, wanted)
    return tail(stats[:2], *ready)


def solution(mesh):
    split = Mesh(mesh.devices.reshape(4, 2, 16, 4), ("x", "c", "z", "y"))
    placed = (P(TOK, VOCAB), P(TOK, VOCAB), P(TOK), P(TOK), P(TOK))
    return jax.shard_map(loss, mesh=split, in_specs=placed, out_specs=(P((*TOK, *VOCAB)), P()), check_vma=False)
```

```python
import jax
import jax.numpy as jnp
from jax import lax
from jax.experimental import pallas as pl
from jax.experimental.pallas import tpu as pltpu
from jax.sharding import Mesh
from jax.sharding import PartitionSpec as P


SEQ_LEN = 128
DOMAINS = 64
TOK = ("x", "c")
VOCAB = ("z", "y")
SWAP = [(0, 1), (1, 0)]
BLOCK = 256
TILE = 256
LONG = 512
LIMIT = 60 << 20
ROUNDS = 8
BATCHES = ((1, 2, 3), (4, 5, 6), (7,))
DEPTHS = (0, 1, 3, 7, 11, 16)


def to_all(array, axis, copies):
    return lax.all_to_all(
        jnp.broadcast_to(array[None], (copies, *array.shape)), axis, 0, 0, tiled=True
    )


def along_z(array):
    zs = lax.axis_size("z")
    pairs = [(c * zs + z, c * zs + (z + (1 - 2 * c)) % zs) for c in range(2) for z in range(zs)]
    return lax.ppermute(array, ("c", "z"), pairs)


def gathered_weight(weight):
    own = to_all(weight, "x", lax.axis_size("x"))
    return own, lax.ppermute(own, "c", SWAP)


def before_tail(tokens, z, y, domains, seq_len):
    zs, ys = lax.axis_size("z"), lax.axis_size("y")
    own = tokens // (zs * ys)
    index = lax.iota(jnp.int32, zs * own)
    local = (index // own) * (ys * own) + y * own + index % own
    sequence = lax.broadcasted_iota(jnp.int32, (zs * own, seq_len.shape[0]), 1)
    of_token = (local // SEQ_LEN)[:, None] == sequence
    lengths = jnp.sum(jnp.where(of_token, seq_len[None], 0), axis=1)
    mask = (local % SEQ_LEN < lengths).astype(jnp.float32)
    place = lax.broadcasted_iota(jnp.int32, (zs, ys, own), 1)
    domain = jnp.sum(jnp.where(place == y, domains.reshape(zs, ys, own), 0), axis=1).reshape(-1)
    here = domain[None, :] == lax.broadcasted_iota(jnp.int32, (DOMAINS, zs * own), 0)
    here = here.astype(jnp.float32)
    outputs = (lax.broadcasted_iota(jnp.int32, (zs, own), 0) == z).astype(jnp.float32)
    return mask, here, outputs, jnp.sum(here * mask[None], axis=1)


def tail(stats, mask, here, outputs, counts):
    zs, ys = lax.axis_size("z"), lax.axis_size("y")
    own = stats.shape[1] // (zs * ys)
    slices = stats.reshape(2, zs, ys, own).transpose(2, 0, 1, 3)
    send = jnp.broadcast_to(slices.reshape(1, ys, -1), (zs, ys, 2 * zs * own))
    got = lax.all_to_all(send.reshape(zs * ys, -1), VOCAB, 0, 0, tiled=True)
    got = got.reshape(zs * ys, 2, zs * own)
    top = jnp.max(got[:, 0], axis=0)
    total = jnp.sum(jnp.exp(got[:, 0] - top[None]), axis=0)
    loss = (jnp.log(total) + top - jnp.sum(got[:, 1], axis=0)) * mask
    sums = jnp.sum(jnp.where(here > 0, loss[None], 0.0), axis=1)
    token_loss = jnp.sum(jnp.where(outputs > 0, loss.reshape(zs, own), 0.0), axis=0)
    part, token_loss = lax.optimization_barrier((jnp.concatenate([sums, counts]), token_loss))
    axes = ("x", "c", "y")
    whole = jnp.sum(to_all(part, axes, lax.axis_size(axes)), axis=0)
    mean = whole[:DOMAINS] / jnp.maximum(whole[DOMAINS:], 1.0)
    return token_loss, mean


def product_kernel(kinds, away):
    def kernel(where, *refs):
        refs = list(refs)
        blocks = []
        for kind in kinds:
            ref = refs.pop(0)
            blocks += [ref.at[k] for k in range(kind)] if kind else [ref]
        own, theirs, wanted, out, acc, rows, lefts, sems = refs
        core, z = where[0], where[1]

        def fetch(k, weights, source):
            return pltpu.make_async_copy(
                weights.at[source // 4, pl.ds(lax.rem(source, 2) * BLOCK, BLOCK)],
                rows.at[pl.ds(k * BLOCK, BLOCK)],
                sems.at[0, k],
            )

        def fetch_block(k):
            return pltpu.make_async_copy(blocks[k], lefts.at[k], sems.at[1, k])

        def begin_fetch(step):
            for k in range(DEPTHS[step], DEPTHS[step + 1]):
                source = lax.rem(z + away[k] * (2 * core - 1) + 16, 16)
                fetch_block(k).start()
                mine = lax.rem(source // 2, 2) == core
                pl.when(mine)(fetch(k, own, source).start)
                pl.when(jnp.logical_not(mine))(fetch(k, theirs, source).start)

        begin_fetch(0)
        begin_fetch(1)
        tokens, columns = acc.shape
        for step, (first, end) in enumerate(zip(DEPTHS, DEPTHS[1:])):
            for k in range(first, end):
                fetch_block(k).wait()
                fetch(k, own, 0).wait()
            if step + 3 < len(DEPTHS):
                begin_fetch(step + 2)
            deep = slice(first * BLOCK, end * BLOCK)
            for at in range(0, tokens, TILE):
                part = slice(at, at + TILE)
                left = jnp.concatenate([lefts[k, part] for k in range(first, end)], axis=1)
                for begin in range(0, columns, LONG):
                    side = slice(begin, begin + LONG)
                    total = jnp.dot(left, rows[deep, side], preferred_element_type=jnp.float32)
                    acc[part, side] = total + acc[part, side] if first else total
                if end < len(away):
                    continue
                values = acc[part]
                top = jnp.max(values, axis=1, keepdims=True)
                total = jnp.sum(jnp.exp(values - top), axis=1, keepdims=True)
                lane = lax.broadcasted_iota(jnp.int32, values.shape, 1)
                picked = jnp.where(lane == wanted[part], values, 0.0)
                picked = jnp.sum(picked, axis=1, keepdims=True)
                lse = jnp.log(total) + top
                lane = lax.broadcasted_iota(jnp.int32, (TILE, 128), 1)
                out[:, part] = jnp.where(lane == 0, lse, picked).T[:2]

    return kernel


def product(where, away, blocks, weights, wanted):
    kinds = [b.shape[0] if b.ndim == 3 else 0 for b in blocks]
    count, tokens, columns = len(away), blocks[0].shape[-2], weights[0].shape[2]
    vmem = pl.BlockSpec(memory_space=pltpu.VMEM)
    hbm = pl.BlockSpec(memory_space=pltpu.HBM)
    return pl.pallas_call(
        product_kernel(kinds, away),
        in_specs=[pl.BlockSpec(memory_space=pltpu.SMEM)] + [hbm] * (len(blocks) + 2) + [vmem],
        out_specs=vmem,
        out_shape=jax.ShapeDtypeStruct((2, tokens), jnp.float32),
        scratch_shapes=[
            pltpu.VMEM((tokens, columns), jnp.float32),
            pltpu.VMEM((count * BLOCK, columns), jnp.bfloat16),
            pltpu.VMEM((count, tokens, BLOCK), jnp.bfloat16),
            pltpu.SemaphoreType.DMA((2, count)),
        ],
        compiler_params=pltpu.CompilerParams(vmem_limit_bytes=LIMIT),
        cost_estimate=pl.CostEstimate(
            flops=2 * count * tokens * BLOCK * columns,
            bytes_accessed=count * BLOCK * (tokens + columns) * 2,
            transcendentals=tokens * columns,
        ),
    )(where, *blocks, *weights, wanted)


def loss(hidden, weight, targets, domains, seq_len):
    ys = lax.axis_size("y")
    core, z, y = (lax.axis_index(name) for name in ("c", "z", "y"))
    low = lax.axis_index(VOCAB) * weight.shape[1]
    hidden, where, z, y, low = lax.optimization_barrier((hidden, jnp.stack([core, z]), z, y, low))
    mine = to_all(hidden.T, "y", ys).reshape(BLOCK, -1).T
    theirs = lax.ppermute(mine, "c", SWAP)
    weights = gathered_weight(weight)
    own, other = [mine], [theirs]
    for r in range(1, ROUNDS + 1):
        own.append(along_z(own[-1]))
        if r == 2:
            domains, seq_len, targets, own[2] = lax.optimization_barrier(
                (domains, seq_len, targets, own[2])
            )
            ready = before_tail(targets.shape[0], z, y, domains, seq_len)
            wanted = (targets - low)[:, None]
        if r == 4:
            own[4], ready, wanted = lax.optimization_barrier((own[4], ready, wanted))
        if r < ROUNDS:
            other.append(along_z(other[-1]))
    swapped = []
    for some in BATCHES:
        swapped.append(lax.ppermute(jnp.stack([other[r] for r in some]), "c", SWAP))
    away = [*range(7), *(-r for some in BATCHES[:2] for r in some), 7, 8, *(-r for r in BATCHES[2])]
    blocks = [*own[:7], *swapped[:2], own[7], own[8], swapped[2]]
    stats = product(where, away, blocks, weights, wanted)
    return tail(stats, *ready)


def solution(mesh):
    split = Mesh(mesh.devices.reshape(4, 2, 16, 4), ("x", "c", "z", "y"))
    placed = (P(TOK, VOCAB), P(TOK, VOCAB), P(TOK), P(TOK), P(TOK))
    return jax.shard_map(loss, mesh=split, in_specs=placed, out_specs=(P((*TOK, *VOCAB)), P()), check_vma=False)
```

```python
import jax
import jax.numpy as jnp
from jax import lax
from jax.experimental import pallas as pl
from jax.experimental.pallas import tpu as pltpu
from jax.sharding import Mesh
from jax.sharding import PartitionSpec as P


SEQ_LEN = 128
DOMAINS = 64
TOK = ("x", "c")
VOCAB = ("z", "y")
SWAP = [(0, 1), (1, 0)]
BLOCK = 256
TILE = 256
LONG = 512
LIMIT = 60 << 20
ROUNDS = 8
BATCHES = ((1, 2, 3), (4, 5, 6), (7,))
DEPTHS = (0, 1, 3, 7, 11, 16)


def to_all(array, axis, copies):
    return lax.all_to_all(
        jnp.broadcast_to(array[None], (copies, *array.shape)), axis, 0, 0, tiled=True
    )


def along_z(array):
    zs = lax.axis_size("z")
    pairs = [(c * zs + z, c * zs + (z + (1 - 2 * c)) % zs) for c in range(2) for z in range(zs)]
    return lax.ppermute(array, ("c", "z"), pairs)


def gathered_weight(weight):
    own = to_all(weight, "x", lax.axis_size("x"))
    return own, lax.ppermute(own, "c", SWAP)


def before_tail(tokens, z, y, domains, seq_len):
    zs, ys = lax.axis_size("z"), lax.axis_size("y")
    own = tokens // (zs * ys)
    index = lax.iota(jnp.int32, zs * own)
    local = (index // own) * (ys * own) + y * own + index % own
    sequence = lax.broadcasted_iota(jnp.int32, (zs * own, seq_len.shape[0]), 1)
    of_token = (local // SEQ_LEN)[:, None] == sequence
    lengths = jnp.sum(jnp.where(of_token, seq_len[None], 0), axis=1)
    mask = (local % SEQ_LEN < lengths).astype(jnp.float32)
    place = lax.broadcasted_iota(jnp.int32, (zs, ys, own), 1)
    domain = jnp.sum(jnp.where(place == y, domains.reshape(zs, ys, own), 0), axis=1).reshape(-1)
    here = domain[None, :] == lax.broadcasted_iota(jnp.int32, (DOMAINS, zs * own), 0)
    here = here.astype(jnp.float32)
    outputs = (lax.broadcasted_iota(jnp.int32, (zs, own), 0) == z).astype(jnp.float32)
    return mask, here, outputs, jnp.sum(here * mask[None], axis=1)


def tail(stats, mask, here, outputs, counts):
    zs, ys = lax.axis_size("z"), lax.axis_size("y")
    own = stats.shape[1] // (zs * ys)
    slices = stats.reshape(2, zs, ys, own).transpose(2, 0, 1, 3)
    send = jnp.broadcast_to(slices.reshape(1, ys, -1), (zs, ys, 2 * zs * own))
    got = lax.all_to_all(send.reshape(zs * ys, -1), VOCAB, 0, 0, tiled=True)
    got = got.reshape(zs * ys, 2, zs * own)
    top = jnp.max(got[:, 0], axis=0)
    total = jnp.sum(jnp.exp(got[:, 0] - top[None]), axis=0)
    loss = (jnp.log(total) + top - jnp.sum(got[:, 1], axis=0)) * mask
    sums = jnp.sum(jnp.where(here > 0, loss[None], 0.0), axis=1)
    token_loss = jnp.sum(jnp.where(outputs > 0, loss.reshape(zs, own), 0.0), axis=0)
    part = jnp.concatenate([sums, counts])
    axes = ("x", "c", "y")
    whole = jnp.sum(to_all(part, axes, lax.axis_size(axes)), axis=0)
    mean = whole[:DOMAINS] / jnp.maximum(whole[DOMAINS:], 1.0)
    return token_loss, mean


def product_kernel(kinds, away):
    def kernel(where, *refs):
        refs = list(refs)
        blocks = []
        for kind in kinds:
            ref = refs.pop(0)
            blocks += [ref.at[k] for k in range(kind)] if kind else [ref]
        own, theirs, wanted, out, acc, rows, lefts, sems = refs
        core, z = where[0], where[1]

        def fetch(k, weights, source):
            return pltpu.make_async_copy(
                weights.at[source // 4, pl.ds(lax.rem(source, 2) * BLOCK, BLOCK)],
                rows.at[pl.ds(k * BLOCK, BLOCK)],
                sems.at[0, k],
            )

        def fetch_block(k):
            return pltpu.make_async_copy(blocks[k], lefts.at[k], sems.at[1, k])

        def begin_fetch(step):
            for k in range(DEPTHS[step], DEPTHS[step + 1]):
                source = lax.rem(z + away[k] * (2 * core - 1) + 16, 16)
                fetch_block(k).start()
                mine = lax.rem(source // 2, 2) == core
                pl.when(mine)(fetch(k, own, source).start)
                pl.when(jnp.logical_not(mine))(fetch(k, theirs, source).start)

        begin_fetch(0)
        begin_fetch(1)
        tokens, columns = acc.shape
        for step, (first, end) in enumerate(zip(DEPTHS, DEPTHS[1:])):
            for k in range(first, end):
                fetch_block(k).wait()
                fetch(k, own, 0).wait()
            if step + 3 < len(DEPTHS):
                begin_fetch(step + 2)
            deep = slice(first * BLOCK, end * BLOCK)
            for at in range(0, tokens, TILE):
                part = slice(at, at + TILE)
                left = jnp.concatenate([lefts[k, part] for k in range(first, end)], axis=1)
                for begin in range(0, columns, LONG):
                    side = slice(begin, begin + LONG)
                    total = jnp.dot(left, rows[deep, side], preferred_element_type=jnp.float32)
                    acc[part, side] = total + acc[part, side] if first else total
                if end < len(away):
                    continue
                values = acc[part]
                top = jnp.max(values, axis=1, keepdims=True)
                total = jnp.sum(jnp.exp(values - top), axis=1, keepdims=True)
                lane = lax.broadcasted_iota(jnp.int32, values.shape, 1)
                picked = jnp.where(lane == wanted[part], values, 0.0)
                picked = jnp.sum(picked, axis=1, keepdims=True)
                lse = jnp.log(total) + top
                lane = lax.broadcasted_iota(jnp.int32, (TILE, 128), 1)
                out[:, part] = jnp.where(lane == 0, lse, picked).T[:2]

    return kernel


def product(where, away, blocks, weights, wanted):
    kinds = [b.shape[0] if b.ndim == 3 else 0 for b in blocks]
    count, tokens, columns = len(away), blocks[0].shape[-2], weights[0].shape[2]
    vmem = pl.BlockSpec(memory_space=pltpu.VMEM)
    hbm = pl.BlockSpec(memory_space=pltpu.HBM)
    return pl.pallas_call(
        product_kernel(kinds, away),
        in_specs=[pl.BlockSpec(memory_space=pltpu.SMEM)] + [hbm] * (len(blocks) + 2) + [vmem],
        out_specs=vmem,
        out_shape=jax.ShapeDtypeStruct((2, tokens), jnp.float32),
        scratch_shapes=[
            pltpu.VMEM((tokens, columns), jnp.float32),
            pltpu.VMEM((count * BLOCK, columns), jnp.bfloat16),
            pltpu.VMEM((count, tokens, BLOCK), jnp.bfloat16),
            pltpu.SemaphoreType.DMA((2, count)),
        ],
        compiler_params=pltpu.CompilerParams(vmem_limit_bytes=LIMIT),
        cost_estimate=pl.CostEstimate(
            flops=2 * count * tokens * BLOCK * columns,
            bytes_accessed=count * BLOCK * (tokens + columns) * 2,
            transcendentals=tokens * columns,
        ),
    )(where, *blocks, *weights, wanted)


def loss(hidden, weight, targets, domains, seq_len):
    ys = lax.axis_size("y")
    core, z, y = (lax.axis_index(name) for name in ("c", "z", "y"))
    low = lax.axis_index(VOCAB) * weight.shape[1]
    hidden, core, z, y, low = lax.optimization_barrier((hidden, core, z, y, low))
    mine = to_all(hidden.T, "y", ys).reshape(BLOCK, -1).T
    theirs = lax.ppermute(mine, "c", SWAP)
    weights = gathered_weight(weight)
    own, other = [mine], [theirs]
    for r in range(1, ROUNDS + 1):
        own.append(along_z(own[-1]))
        if r == 2:
            domains, seq_len, targets, own[2] = lax.optimization_barrier(
                (domains, seq_len, targets, own[2])
            )
            ready = before_tail(targets.shape[0], z, y, domains, seq_len)
            wanted = (targets - low)[:, None]
            where = jnp.where(lax.iota(jnp.int32, 2) == 0, core, z)
        if r == 4:
            own[4], ready, wanted, where = lax.optimization_barrier(
                (own[4], ready, wanted, where)
            )
        if r < ROUNDS:
            other.append(along_z(other[-1]))
    swapped = []
    for some in BATCHES:
        swapped.append(lax.ppermute(jnp.stack([other[r] for r in some]), "c", SWAP))
    away = [*range(7), *(-r for some in BATCHES[:2] for r in some), 7, 8, *(-r for r in BATCHES[2])]
    blocks = [*own[:7], *swapped[:2], own[7], own[8], swapped[2]]
    stats = product(where, away, blocks, weights, wanted)
    return tail(stats, *ready)


def solution(mesh):
    split = Mesh(mesh.devices.reshape(4, 2, 16, 4), ("x", "c", "z", "y"))
    placed = (P(TOK, VOCAB), P(TOK, VOCAB), P(TOK), P(TOK), P(TOK))
    return jax.shard_map(loss, mesh=split, in_specs=placed, out_specs=(P((*TOK, *VOCAB)), P()), check_vma=False)
```
